32 devices in a mesh: kv: 2 (over core), seq: 16 (over z, y, x), dp: 1.
Axes of the slice: x: 2, y: 2, z: 4, core: 2. Of those that a mesh axis runs over, the one named last changes fastest.
Arguments:
- token_input_state: bfloat16 [4, 8192], P('dp'), may hold values from -6 to 6
- query_matrix: bfloat16 [8192, 2048], P('seq', 'kv'), may hold values from -0.0625 to 0.0625
- key_value_weight: bfloat16 [8192, 512], P('seq', 'kv'), may hold values from -0.5 to 0.5
- output_weight: bfloat16 [2048, 8192], P('kv', 'seq'), may hold values from -0.125 to 0.125
- key_cache_rows: bfloat16 [4, 2, 32768, 128], P('dp', 'kv', 'seq'), may hold values from -6000 to 6000, as said below
- value_cache_rows: bfloat16 [4, 2, 32768, 128], P('dp', 'kv', 'seq'), may hold values from -24 to 24
- live_lengths: int32 [4, 16], P('dp'), may hold values from 2 to 2048, as said below
- owner_shard: int32 [4], P('dp'), may hold values from 0 to 15
Outputs:
- layer_out: bfloat16 [4, 8192], P('dp', 'seq')
The draws below stay inside these ranges and needn't reach their ends.
Inputs may be any that keep to these rules, and one draw needn't show every extreme that they name: `live_lengths`: every block holds 2 to 2048 live slots; the owner's block of a sequence holds fewer than 2048; in every sequence some other block holds exactly 2048. `key_cache_rows`: bounded as stated.
All inputs are finite; a program needn't handle non-finite values.
Results may differ from the reference program's by a relative error of at most 0.015.
The reference program's roundings to bfloat16 on the way (of `attended`) count: a program that leaves them out, or rounds other values in their place, can miss the bound.
Values may be sent and summed in bfloat16 or wider, within the bound.
A program may use at most 64 MiB of HBM per device.

```python
import math
import jax
import jax.numpy as jnp
from jax import lax

MODEL_WIDTH = 8192
HEAD_SIZE = 128
QUERY_GROUP = 8
BATCH_SEQUENCES = 4
LENGTH_PER_PART = 2048
KEY_VALUE_HEADS = 2
HQ = 16
CACHE_LENGTH = 32768
N_SEQ = 16


def lengths_and_owner(key):
    inner = jax.random.fold_in(key, 4242)
    first_key, second_key, third_key, fourth_key, fifth_key = jax.random.split(inner, 5)
    owner_shard = jax.random.randint(first_key, (BATCH_SEQUENCES,), 0, N_SEQ)
    owner_shard = jnp.where(jnp.arange(BATCH_SEQUENCES) == 0, N_SEQ - 1, owner_shard)
    first_draw = jax.random.randint(second_key, (BATCH_SEQUENCES, N_SEQ), 0, LENGTH_PER_PART)
    second_draw = jax.random.randint(third_key, (BATCH_SEQUENCES, N_SEQ), 0, LENGTH_PER_PART)
    third_draw = jax.random.randint(fourth_key, (BATCH_SEQUENCES, N_SEQ), 0, LENGTH_PER_PART)
    skewed = first_draw * second_draw // LENGTH_PER_PART * third_draw // LENGTH_PER_PART
    lengths = 2 + skewed
    lengths = jnp.minimum(lengths, LENGTH_PER_PART - 1)
    column = jnp.arange(N_SEQ)[None, :]
    extra = jax.random.randint(fifth_key, (BATCH_SEQUENCES,), 0, N_SEQ - 1)
    full_shard = (owner_shard + 1 + extra) % N_SEQ
    lengths = jnp.where(column == full_shard[:, None], LENGTH_PER_PART, lengths)
    return (lengths.astype(jnp.int32), owner_shard.astype(jnp.int32))


def draw_live_lengths(key, part):
    lengths, owner_shard = lengths_and_owner(key)
    return lengths


def draw_owner_shard(key, part):
    lengths, owner_shard = lengths_and_owner(key)
    return owner_shard


def draw_key_cache_rows(key, part):
    inner = jax.random.fold_in(key, 77)
    noise_key = jax.random.fold_in(inner, 0)
    complete_shape = (BATCH_SEQUENCES, KEY_VALUE_HEADS, N_SEQ, LENGTH_PER_PART, HEAD_SIZE)
    random_basis = jnp.clip(2.5 * jax.random.normal(noise_key, complete_shape, jnp.float32), -15.0, 15.0)
    return random_basis.reshape(BATCH_SEQUENCES, KEY_VALUE_HEADS, CACHE_LENGTH, HEAD_SIZE).astype(jnp.bfloat16)


def block_levels(rng, dims, shards, low, top_value):
    def one(dim, parts):
        steps = jax.random.uniform(jax.random.fold_in(jax.random.fold_in(rng, 6), dim), (parts,), jnp.float32, low / len(shards), top_value / len(shards))
        return jnp.repeat(jnp.exp(steps), dims[dim] // parts).reshape((-1,) + (1,) * (len(dims) - dim - 1))

    loudness = one(*shards[0])
    for cut in shards[1:]:
        loudness = loudness * one(*cut)
    return loudness


def normal_values(rng, shape, deviation, limit, cuts=(), held_as=jnp.bfloat16):
    factor_of = block_levels(rng, shape, cuts, -0.22, 0.18) if cuts else 1.0
    drawn = jax.random.normal(rng, shape, jnp.float32) * deviation * factor_of
    return jnp.minimum(jnp.maximum(drawn, -limit), limit).astype(held_as)


def setup_inputs(seed: int = 0, part: int = 0) -> dict:
    keys = jax.random.split(jax.random.key(seed), 9)
    part_splits = jax.random.split(jax.random.fold_in(keys[8], part), 9)
    token_input_state = normal_values(part_splits[0], (BATCH_SEQUENCES, MODEL_WIDTH), 1.0, 6.0)
    query_matrix = normal_values(keys[1], (MODEL_WIDTH, HQ * HEAD_SIZE), MODEL_WIDTH ** -0.5, 0.0625, ((0, 16), (1, 2)))
    key_value_weight = normal_values(keys[2], (MODEL_WIDTH, KEY_VALUE_HEADS * 2 * HEAD_SIZE), (MODEL_WIDTH // 64) ** -0.5, 0.5, ((0, 16), (1, 2)))
    output_weight = normal_values(keys[3], (HQ * HEAD_SIZE, MODEL_WIDTH), (HQ * HEAD_SIZE) ** -0.5, 0.125, ((0, 2), (1, 16)))
    key_cache_rows = draw_key_cache_rows(jax.random.fold_in(jax.random.fold_in(keys[8], part), 71), part)
    value_cache_rows = normal_values(part_splits[5], (BATCH_SEQUENCES, KEY_VALUE_HEADS, CACHE_LENGTH, HEAD_SIZE), 4.0, 24.0, ((1, 2), (2, 16)))
    live_lengths = draw_live_lengths(jax.random.fold_in(jax.random.fold_in(keys[8], part), 71), part)
    owner_shard = draw_owner_shard(jax.random.fold_in(jax.random.fold_in(keys[8], part), 71), part)
    return {"token_input_state": token_input_state, "query_matrix": query_matrix, "key_value_weight": key_value_weight, "output_weight": output_weight, "key_cache_rows": key_cache_rows, "value_cache_rows": value_cache_rows, "live_lengths": live_lengths, "owner_shard": owner_shard}


rope_theta = 500000.0

def frequencies():
    exponent = jnp.arange(0, HEAD_SIZE, 2).astype(jnp.float32) / HEAD_SIZE
    return jnp.power(rope_theta, -exponent)

def rotate(vectors, angles):
    half_size = vectors.shape[-1] // 2
    first_half = vectors[..., :half_size]
    second_half = vectors[..., half_size:]
    cosine_table = jnp.cos(angles)
    sine_table = jnp.sin(angles)
    return jnp.concatenate([first_half * cosine_table - second_half * sine_table, second_half * cosine_table + first_half * sine_table], -1)

def reference(token_input_state, query_matrix, key_value_weight, output_weight, key_cache_rows, value_cache_rows, live_lengths, owner_shard):
    query_rows = jnp.dot(token_input_state, query_matrix, preferred_element_type=jnp.float32).reshape(BATCH_SEQUENCES, KEY_VALUE_HEADS, QUERY_GROUP, HEAD_SIZE)
    key_value_rows = jnp.dot(token_input_state, key_value_weight, preferred_element_type=jnp.float32).reshape(BATCH_SEQUENCES, KEY_VALUE_HEADS, 2, HEAD_SIZE)
    lookup = jnp.take_along_axis(live_lengths, owner_shard[:, None].astype(jnp.int32), 1)[:, 0]
    position = owner_shard * LENGTH_PER_PART + lookup
    angles = position.astype(jnp.float32)[:, None] * frequencies()[None, :]
    query_rot = rotate(query_rows, angles[:, None, None, :]).astype(jnp.bfloat16)
    key_new = rotate(key_value_rows[:, :, 0], angles[:, None, :]).astype(jnp.bfloat16)
    value_new = key_value_rows[:, :, 1].astype(jnp.bfloat16)
    scaling = 1.0 / math.sqrt(HEAD_SIZE)
    key_rows = key_cache_rows.reshape(BATCH_SEQUENCES, KEY_VALUE_HEADS, N_SEQ, LENGTH_PER_PART, HEAD_SIZE)
    value_rows = value_cache_rows.reshape(BATCH_SEQUENCES, KEY_VALUE_HEADS, N_SEQ, LENGTH_PER_PART, HEAD_SIZE)
    scores = jnp.einsum('bhgd,bhsld->bhgsl', query_rot.astype(jnp.float32), key_rows.astype(jnp.float32)) * scaling
    slot_ids = jnp.arange(LENGTH_PER_PART)
    live_mask = slot_ids[None, None, :] < live_lengths[:, :, None]
    scores = jnp.where(live_mask[:, None, None], scores, -jnp.inf)
    new_score = lax.optimization_barrier(jnp.sum(query_rot.astype(jnp.float32) * key_new.astype(jnp.float32)[:, :, None, :], -1)) * scaling
    owner_mask = (owner_shard[:, None] == jnp.arange(N_SEQ)[None, :])[:, None, None, :]
    new_term = jnp.where(owner_mask, new_score[..., None], -jnp.inf)
    shard_top = jnp.maximum(lax.optimization_barrier(jnp.max(scores, -1)), new_term)
    probs = jnp.exp(scores - shard_top[..., None]).astype(jnp.bfloat16)
    new_prob = jnp.where(owner_mask, jnp.exp(new_score[..., None] - shard_top), 0.0).astype(jnp.bfloat16)
    totals = lax.optimization_barrier(jnp.sum(probs.astype(jnp.float32), -1)) + new_prob.astype(jnp.float32)
    accum = jnp.einsum('bhgsl,bhsld->bhgsd', probs.astype(jnp.float32), value_rows.astype(jnp.float32))
    accum = accum + new_prob.astype(jnp.float32)[..., None] * value_new.astype(jnp.float32)[:, :, None, None, :]
    overall = lax.optimization_barrier(jnp.max(shard_top, -1))
    factor = jnp.exp(shard_top - overall[..., None])
    attended = lax.optimization_barrier(jnp.sum(accum * factor[..., None], 3)) / lax.optimization_barrier(jnp.sum(totals * factor, 3))[..., None]
    attended = attended.astype(jnp.bfloat16).reshape(BATCH_SEQUENCES, HQ * HEAD_SIZE)
    return jnp.dot(attended, output_weight, preferred_element_type=jnp.float32).astype(jnp.bfloat16)
```

```python
import functools
import math

import jax
import jax.numpy as jnp
import numpy as np
from jax import lax
from jax.experimental import pallas as pl
from jax.experimental.pallas import tpu as pltpu
from jax.sharding import PartitionSpec as P

ROPE_THETA = 500000.0
F32 = jnp.float32
BF16 = jnp.bfloat16


def gather_start(buf, rank, count, send_sem, recv_sem, peer_of):
    copies = []
    for d in range(1, count):
        j = lax.rem(rank + d, count)
        cp = pltpu.make_async_remote_copy(
            src_ref=buf.at[rank],
            dst_ref=buf.at[rank],
            send_sem=send_sem.at[d],
            recv_sem=recv_sem.at[rank],
            device_id=peer_of(j),
            device_id_type=pl.DeviceIdType.MESH,
        )
        cp.start()
        copies.append(cp)
    return copies


def gather_wait(buf, rank, count, send_sem, recv_sem, peer_of):
    for d in range(1, count):
        j = lax.rem(rank + d, count)
        pltpu.make_async_remote_copy(
            src_ref=buf.at[j],
            dst_ref=buf.at[j],
            send_sem=send_sem.at[d],
            recv_sem=recv_sem.at[j],
            device_id=peer_of(j),
            device_id_type=pl.DeviceIdType.MESH,
        ).wait_recv()


def kernel(
    inner, outer, kv_size, group, head,
    live, owner, freq, x_hbm, wq_hbm, wkv_hbm, wo_hbm, k_hbm, v_hbm,
    out,
    x, wq, wkv, wo, keys, vals,
    part_in, part_out, acc_in, acc_out, kv_buf, q_rows, att_rows,
    load_sem, sa, ra, sb, rb, sc, rc, sd, rd, se, re,
):
    me = lax.axis_index("seq")
    kv = lax.axis_index("kv")
    batch = x.shape[0]
    rows = wq.shape[0]
    qw = wq.shape[1]
    slots = keys.shape[2]
    plane = me // inner
    spot = lax.rem(me, inner)

    def inner_peer(j):
        return {"seq": plane * inner + j}

    def outer_peer(j):
        return {"seq": j * inner + spot}

    def kv_peer(j):
        return {"kv": j}

    barrier = pltpu.get_barrier_semaphore()
    for d in range(1, inner):
        pl.semaphore_signal(barrier, inc=1, device_id=inner_peer(lax.rem(spot + d, inner)),
                            device_id_type=pl.DeviceIdType.MESH)
    for d in range(1, outer):
        pl.semaphore_signal(barrier, inc=1, device_id=outer_peer(lax.rem(plane + d, outer)),
                            device_id_type=pl.DeviceIdType.MESH)
    for d in range(1, kv_size):
        pl.semaphore_signal(barrier, inc=1, device_id=kv_peer(lax.rem(kv + d, kv_size)),
                            device_id_type=pl.DeviceIdType.MESH)

    first = pl.multiple_of(me * rows, rows)
    loads = [
        pltpu.make_async_copy(x_hbm.at[:, pl.ds(first, rows)], x, load_sem.at[0]),
        pltpu.make_async_copy(wq_hbm, wq, load_sem.at[1]),
        pltpu.make_async_copy(wkv_hbm, wkv, load_sem.at[2]),
        pltpu.make_async_copy(k_hbm, keys, load_sem.at[3]),
        pltpu.make_async_copy(v_hbm, vals, load_sem.at[4]),
        pltpu.make_async_copy(wo_hbm, wo, load_sem.at[5]),
    ]
    for cp in loads:
        cp.start()

    row_id = lax.broadcasted_iota(jnp.int32, (batch, head), 0)
    lane_id = lax.broadcasted_iota(jnp.int32, (batch, head), 1)
    position = jnp.zeros((batch, head), jnp.int32)
    for b in range(batch):
        own = owner[b]
        position = jnp.where(row_id == b, own * slots + live[b, own], position)
    angle = position.astype(F32) * freq[...]
    cosine = jnp.cos(angle)
    sine = jnp.sin(angle)
    sine = jnp.where(lane_id < head // 2, -sine, sine)

    def rotate(v):
        return v * cosine + pltpu.roll(v, head // 2, 1) * sine

    for cp in loads[:3]:
        cp.wait()
    xs = x[...]
    part_in[spot, :, :qw] = jnp.dot(xs, wq[...], preferred_element_type=F32)
    part_in[spot, :, qw:] = jnp.dot(xs, wkv[...], preferred_element_type=F32)
    pl.semaphore_wait(barrier, inner + outer + kv_size - 3)

    sends = gather_start(part_in, spot, inner, sa, ra, inner_peer)
    gather_wait(part_in, spot, inner, sa, ra, inner_peer)
    total = part_in[0]
    for j in range(1, inner):
        total = total + part_in[j]
    part_out[plane] = total
    sends += gather_start(part_out, plane, outer, sb, rb, outer_peer)
    gather_wait(part_out, plane, outer, sb, rb, outer_peer)
    total = part_out[0]
    for j in range(1, outer):
        total = total + part_out[j]

    for h in range(group):
        q_rows[:, h, :] = rotate(total[:, h * head:(h + 1) * head])
    key_new = rotate(total[:, qw:qw + head]).astype(BF16).astype(F32)
    value_new = total[:, qw + head:qw + 2 * head].astype(BF16).astype(F32)

    loads[3].wait()
    loads[4].wait()
    scaling = 1.0 / math.sqrt(head)
    slot_id = lax.broadcasted_iota(jnp.int32, (group, slots), 1)
    stat_lane = lax.broadcasted_iota(jnp.int32, (group, head), 1)
    stat = jnp.zeros((group, head), F32)
    for b in range(batch):
        q = q_rows[b].astype(BF16)
        new_score = jnp.sum(q.astype(F32) * key_new[b:b + 1], -1, keepdims=True) * scaling
        new_score = jnp.where(owner[b] == me, new_score, -jnp.inf)
        s = lax.dot_general(q, keys[b, 0], (((1,), (1,)), ((), ())), preferred_element_type=F32)
        s = jnp.where(slot_id < live[b, me], s * scaling, -jnp.inf)
        top = jnp.maximum(jnp.max(s, -1, keepdims=True), new_score)
        prob = jnp.exp(s - top).astype(BF16)
        new_prob = jnp.exp(new_score - top).astype(BF16).astype(F32)
        count = jnp.sum(prob.astype(F32), -1, keepdims=True) + new_prob
        acc = jnp.dot(prob, vals[b, 0], preferred_element_type=F32)
        acc_in[spot, b * group:(b + 1) * group] = acc + new_prob * value_new[b:b + 1]
        stat = jnp.where(stat_lane == b, top, stat)
        stat = jnp.where(stat_lane == batch + b, count, stat)
    acc_in[spot, batch * group:] = stat

    def merge(buf, members):
        stats = [buf[j, batch * group:] for j in range(members)]
        top = stats[0]
        for t in stats[1:]:
            top = jnp.maximum(top, t)
        factors = [jnp.exp(jnp.where(stat_lane < batch, t - top, 0.0)) for t in stats]
        count = None
        for f, t in zip(factors, stats):
            term = f * pltpu.roll(t, head - batch, 1)
            count = term if count is None else count + term
        sums = []
        for b in range(batch):
            acc = None
            for j in range(members):
                term = factors[j][:, b:b + 1] * buf[j, b * group:(b + 1) * group]
                acc = term if acc is None else acc + term
            sums.append(acc)
        return top, count, sums

    sends += gather_start(acc_in, spot, inner, sc, rc, inner_peer)
    gather_wait(acc_in, spot, inner, sc, rc, inner_peer)
    top, count, sums = merge(acc_in, inner)
    for b in range(batch):
        acc_out[plane, b * group:(b + 1) * group] = sums[b]
    acc_out[plane, batch * group:] = jnp.where(stat_lane < batch, top, pltpu.roll(count, batch, 1))
    sends += gather_start(acc_out, plane, outer, sd, rd, outer_peer)
    gather_wait(acc_out, plane, outer, sd, rd, outer_peer)
    top, count, sums = merge(acc_out, outer)
    for b in range(batch):
        att_rows[b] = sums[b] / count[:, b:b + 1]
    attended = jnp.concatenate([att_rows[:, h, :].astype(BF16) for h in range(group)], -1)

    loads[5].wait()
    kv_buf[kv] = jnp.dot(attended, wo[...], preferred_element_type=F32)
    sends += gather_start(kv_buf, kv, kv_size, se, re, kv_peer)
    gather_wait(kv_buf, kv, kv_size, se, re, kv_peer)
    total = kv_buf[0]
    for j in range(1, kv_size):
        total = total + kv_buf[j]
    out[...] = total.astype(BF16)
    for cp in sends:
        cp.wait_send()


def local(n, kv_size, x, wq, wkv, wo, keys, vals, live, owner):
    batch = x.shape[0]
    head = keys.shape[3]
    rows, qw = wq.shape
    group = qw // head
    cols = wo.shape[1]
    inner = 1
    while inner * inner < n and n % (inner * 2) == 0:
        inner *= 2
    outer = n // inner
    half = np.float64(ROPE_THETA) ** (-np.arange(0, head, 2, dtype=np.float64) / head)
    freq = jnp.asarray(np.concatenate([half, half]).astype(np.float32)[None, :])
    dma = pltpu.SemaphoreType.DMA
    acc_rows = batch * group + group
    smem = pl.BlockSpec(memory_space=pltpu.SMEM)
    vmem = pl.BlockSpec(memory_space=pltpu.VMEM)
    hbm = pl.BlockSpec(memory_space=pl.ANY)
    return pl.pallas_call(
        functools.partial(kernel, inner, outer, kv_size, group, head),
        out_shape=jax.ShapeDtypeStruct((batch, cols), BF16),
        in_specs=[smem, smem, vmem] + [hbm] * 6,
        out_specs=vmem,
        scratch_shapes=[
            pltpu.VMEM((batch, rows), BF16),
            pltpu.VMEM(wq.shape, BF16),
            pltpu.VMEM(wkv.shape, BF16),
            pltpu.VMEM(wo.shape, BF16),
            pltpu.VMEM(keys.shape, BF16),
            pltpu.VMEM(vals.shape, BF16),
            pltpu.VMEM((inner, batch, qw + wkv.shape[1]), F32),
            pltpu.VMEM((outer, batch, qw + wkv.shape[1]), F32),
            pltpu.VMEM((inner, acc_rows, head), F32),
            pltpu.VMEM((outer, acc_rows, head), F32),
            pltpu.VMEM((kv_size, batch, cols), F32),
            pltpu.VMEM((batch, group, head), F32),
            pltpu.VMEM((batch, group, head), F32),
            dma((6,)),
            dma((inner,)), dma((inner,)),
            dma((outer,)), dma((outer,)),
            dma((inner,)), dma((inner,)),
            dma((outer,)), dma((outer,)),
            dma((kv_size,)), dma((kv_size,)),
        ],
        compiler_params=pltpu.CompilerParams(collective_id=0, has_side_effects=True),
    )(live, owner, freq, x, wq, wkv, wo, keys, vals)


def solution(mesh):
    return jax.shard_map(
        functools.partial(local, mesh.shape["seq"], mesh.shape["kv"]),
        mesh=mesh,
        in_specs=(
            P("dp", None),
            P("seq", "kv"),
            P("seq", "kv"),
            P("kv", "seq"),
            P("dp", "kv", "seq", None),
            P("dp", "kv", "seq", None),
            P("dp", None),
            P("dp"),
        ),
        out_specs=P("dp", "seq"),
        check_vma=False,
    )
```

```python
import functools
import math

import jax
import jax.numpy as jnp
import numpy as np
from jax import lax
from jax.experimental import pallas as pl
from jax.experimental.pallas import tpu as pltpu
from jax.sharding import PartitionSpec as P

ROPE_THETA = 500000.0
F32 = jnp.float32
BF16 = jnp.bfloat16


def gather_start(buf, rank, count, send_sem, recv_sem, peer_of):
    copies = []
    for d in range(1, count):
        j = lax.rem(rank + d, count)
        cp = pltpu.make_async_remote_copy(
            src_ref=buf.at[rank],
            dst_ref=buf.at[rank],
            send_sem=send_sem.at[d],
            recv_sem=recv_sem.at[rank],
            device_id=peer_of(j),
            device_id_type=pl.DeviceIdType.MESH,
        )
        cp.start()
        copies.append(cp)
    return copies


def gather_wait(buf, rank, count, send_sem, recv_sem, peer_of):
    for d in range(1, count):
        j = lax.rem(rank + d, count)
        pltpu.make_async_remote_copy(
            src_ref=buf.at[j],
            dst_ref=buf.at[j],
            send_sem=send_sem.at[d],
            recv_sem=recv_sem.at[j],
            device_id=peer_of(j),
            device_id_type=pl.DeviceIdType.MESH,
        ).wait_recv()


def kernel(
    inner, outer, kv_size, group, head,
    live, owner, freq, x_hbm, wq_hbm, wkv_hbm, wo_hbm, k_hbm, v_hbm,
    out,
    x, wq, wkv, wo, keys, vals,
    qa_in, qa_out, qb_in, qb_out, aa_in, aa_out, ab_in, ab_out, kv_buf, q_rows, att_rows,
    load_sem, inner_sem, outer_sem, kv_sem,
):
    me = lax.axis_index("seq")
    kv = lax.axis_index("kv")
    batch = x.shape[0]
    rows = wq.shape[0]
    qw = wq.shape[1]
    slots = keys.shape[2]
    plane = me // inner
    spot = lax.rem(me, inner)

    def inner_peer(j):
        return {"seq": plane * inner + j}

    def outer_peer(j):
        return {"seq": j * inner + spot}

    def kv_peer(j):
        return {"kv": j}

    barrier = pltpu.get_barrier_semaphore()
    for d in range(1, inner):
        pl.semaphore_signal(barrier, inc=1, device_id=inner_peer(lax.rem(spot + d, inner)),
                            device_id_type=pl.DeviceIdType.MESH)
    for d in range(1, outer):
        pl.semaphore_signal(barrier, inc=1, device_id=outer_peer(lax.rem(plane + d, outer)),
                            device_id_type=pl.DeviceIdType.MESH)
    for d in range(1, kv_size):
        pl.semaphore_signal(barrier, inc=1, device_id=kv_peer(lax.rem(kv + d, kv_size)),
                            device_id_type=pl.DeviceIdType.MESH)

    first = pl.multiple_of(me * rows, rows)
    loads = [
        pltpu.make_async_copy(x_hbm.at[:, pl.ds(first, rows)], x, load_sem.at[0]),
        pltpu.make_async_copy(wq_hbm, wq, load_sem.at[1]),
        pltpu.make_async_copy(wkv_hbm, wkv, load_sem.at[2]),
        pltpu.make_async_copy(k_hbm, keys, load_sem.at[3]),
        pltpu.make_async_copy(v_hbm, vals, load_sem.at[4]),
        pltpu.make_async_copy(wo_hbm, wo, load_sem.at[5]),
    ]
    for cp in loads[:3]:
        cp.start()

    sends = []

    def inner_start(buf, i):
        sends.extend(gather_start(buf, spot, inner, inner_sem.at[2 * i], inner_sem.at[2 * i + 1], inner_peer))

    def inner_wait(buf, i):
        gather_wait(buf, spot, inner, inner_sem.at[2 * i], inner_sem.at[2 * i + 1], inner_peer)

    def outer_start(buf, i):
        sends.extend(gather_start(buf, plane, outer, outer_sem.at[2 * i], outer_sem.at[2 * i + 1], outer_peer))

    def outer_wait(buf, i):
        gather_wait(buf, plane, outer, outer_sem.at[2 * i], outer_sem.at[2 * i + 1], outer_peer)

    def add_up(buf, members):
        total = buf[0]
        for j in range(1, members):
            total = total + buf[j]
        return total

    row_id = lax.broadcasted_iota(jnp.int32, (batch, head), 0)
    lane_id = lax.broadcasted_iota(jnp.int32, (batch, head), 1)
    position = jnp.zeros((batch, head), jnp.int32)
    for b in range(batch):
        own = owner[b]
        position = jnp.where(row_id == b, own * slots + live[b, own], position)
    angle = position.astype(F32) * freq[...]
    cosine = jnp.cos(angle)
    sine = jnp.sin(angle)
    sine = jnp.where(lane_id < head // 2, -sine, sine)

    def rotate(v):
        return v * cosine + pltpu.roll(v, head // 2, 1) * sine

    for cp in loads[:3]:
        cp.wait()
    for cp in loads[3:]:
        cp.start()
    xs = x[...]
    cut = qa_in.shape[2]
    qa_in[spot] = jnp.dot(xs, wq[:, :cut], preferred_element_type=F32)
    qb_out[plane, :, :qw - cut] = jnp.dot(xs, wq[:, cut:], preferred_element_type=F32)
    qb_out[plane, :, qw - cut:] = jnp.dot(xs, wkv[...], preferred_element_type=F32)
    pl.semaphore_wait(barrier, inner + outer + kv_size - 3)

    inner_start(qa_in, 0)
    outer_start(qb_out, 0)
    inner_wait(qa_in, 0)
    qa_out[plane] = add_up(qa_in, inner)
    outer_start(qa_out, 1)
    outer_wait(qb_out, 0)
    qb_in[spot] = add_up(qb_out, outer)
    inner_start(qb_in, 1)
    outer_wait(qa_out, 1)
    inner_wait(qb_in, 1)
    total = jnp.concatenate([add_up(qa_out, outer), add_up(qb_in, inner)], -1)

    for h in range(group):
        q_rows[:, h, :] = rotate(total[:, h * head:(h + 1) * head])
    key_new = rotate(total[:, qw:qw + head]).astype(BF16).astype(F32)
    value_new = total[:, qw + head:qw + 2 * head].astype(BF16).astype(F32)

    loads[3].wait()
    loads[4].wait()
    scaling = 1.0 / math.sqrt(head)
    slot_id = lax.broadcasted_iota(jnp.int32, (group, slots), 1)
    stat_lane = lax.broadcasted_iota(jnp.int32, (group, head), 1)

    def attend(b):
        q = q_rows[b].astype(BF16)
        new_score = jnp.sum(q.astype(F32) * key_new[b:b + 1], -1, keepdims=True) * scaling
        new_score = jnp.where(owner[b] == me, new_score, -jnp.inf)
        s = lax.dot_general(q, keys[b, 0], (((1,), (1,)), ((), ())), preferred_element_type=F32)
        s = jnp.where(slot_id < live[b, me], s * scaling, -jnp.inf)
        top = jnp.maximum(jnp.max(s, -1, keepdims=True), new_score)
        prob = jnp.exp(s - top).astype(BF16)
        new_prob = jnp.exp(new_score - top).astype(BF16).astype(F32)
        count = jnp.sum(prob.astype(F32), -1, keepdims=True) + new_prob
        acc = jnp.dot(prob, vals[b, 0], preferred_element_type=F32)
        return top, count, acc + new_prob * value_new[b:b + 1]

    def attend_half(buf, slot, ids):
        nb = len(ids)
        stat = jnp.zeros((group, head), F32)
        for i, b in enumerate(ids):
            top, count, acc = attend(b)
            buf[slot, i * group:(i + 1) * group] = acc
            stat = jnp.where(stat_lane == i, top, stat)
            stat = jnp.where(stat_lane == nb + i, count, stat)
        buf[slot, nb * group:] = stat

    def merge(buf, members):
        nb = buf.shape[1] // group - 1
        stats = [buf[j, nb * group:] for j in range(members)]
        top = stats[0]
        for t in stats[1:]:
            top = jnp.maximum(top, t)
        factors = [jnp.exp(jnp.where(stat_lane < nb, t - top, 0.0)) for t in stats]
        count = None
        for f, t in zip(factors, stats):
            term = f * pltpu.roll(t, head - nb, 1)
            count = term if count is None else count + term
        sums = []
        for b in range(nb):
            acc = None
            for j in range(members):
                term = factors[j][:, b:b + 1] * buf[j, b * group:(b + 1) * group]
                acc = term if acc is None else acc + term
            sums.append(acc)
        return top, count, sums

    def merge_into(buf, members, dst, slot):
        nb = buf.shape[1] // group - 1
        top, count, sums = merge(buf, members)
        for b in range(nb):
            dst[slot, b * group:(b + 1) * group] = sums[b]
        dst[slot, nb * group:] = jnp.where(stat_lane < nb, top, pltpu.roll(count, nb, 1))

    def finish(buf, members, ids):
        top, count, sums = merge(buf, members)
        for i, b in enumerate(ids):
            att_rows[b] = sums[i] / count[:, i:i + 1]

    ids_a = list(range(batch // 2))
    ids_b = list(range(batch // 2, batch))
    attend_half(ab_out, plane, ids_b)
    outer_start(ab_out, 2)
    attend_half(aa_in, spot, ids_a)
    inner_start(aa_in, 2)
    inner_wait(aa_in, 2)
    merge_into(aa_in, inner, aa_out, plane)
    outer_start(aa_out, 3)
    outer_wait(ab_out, 2)
    merge_into(ab_out, outer, ab_in, spot)
    inner_start(ab_in, 3)
    inner_wait(ab_in, 3)
    finish(ab_in, inner, ids_b)
    outer_wait(aa_out, 3)
    finish(aa_out, outer, ids_a)
    attended = jnp.concatenate([att_rows[:, h, :].astype(BF16) for h in range(group)], -1)

    loads[5].wait()
    kv_buf[kv] = jnp.dot(attended, wo[...], preferred_element_type=F32)
    sends.extend(gather_start(kv_buf, kv, kv_size, kv_sem.at[0], kv_sem.at[1], kv_peer))
    gather_wait(kv_buf, kv, kv_size, kv_sem.at[0], kv_sem.at[1], kv_peer)
    out[...] = add_up(kv_buf, kv_size)
    for cp in sends:
        cp.wait_send()


def local(n, kv_size, x, wq, wkv, wo, keys, vals, live, owner):
    batch = x.shape[0]
    head = keys.shape[3]
    rows, qw = wq.shape
    group = qw // head
    cols = wo.shape[1]
    inner = 1
    while inner * inner < n and n % (inner * 2) == 0:
        inner *= 2
    outer = n // inner
    half = np.float64(ROPE_THETA) ** (-np.arange(0, head, 2, dtype=np.float64) / head)
    freq = jnp.asarray(np.concatenate([half, half]).astype(np.float32)[None, :])
    dma = pltpu.SemaphoreType.DMA
    width = qw + wkv.shape[1]
    cut = width // (2 * head) * head
    rows_a = (batch // 2 + 1) * group
    rows_b = (batch - batch // 2 + 1) * group
    smem = pl.BlockSpec(memory_space=pltpu.SMEM)
    vmem = pl.BlockSpec(memory_space=pltpu.VMEM)
    hbm = pl.BlockSpec(memory_space=pl.ANY)
    return pl.pallas_call(
        functools.partial(kernel, inner, outer, kv_size, group, head),
        out_shape=pltpu.VMEM((batch, cols), F32),
        in_specs=[smem, smem, vmem] + [hbm] * 6,
        out_specs=vmem,
        scratch_shapes=[
            pltpu.VMEM((batch, rows), BF16),
            pltpu.VMEM(wq.shape, BF16),
            pltpu.VMEM(wkv.shape, BF16),
            pltpu.VMEM(wo.shape, BF16),
            pltpu.VMEM(keys.shape, BF16),
            pltpu.VMEM(vals.shape, BF16),
            pltpu.VMEM((inner, batch, cut), F32),
            pltpu.VMEM((outer, batch, cut), F32),
            pltpu.VMEM((inner, batch, width - cut), F32),
            pltpu.VMEM((outer, batch, width - cut), F32),
            pltpu.VMEM((inner, rows_a, head), F32),
            pltpu.VMEM((outer, rows_a, head), F32),
            pltpu.VMEM((inner, rows_b, head), F32),
            pltpu.VMEM((outer, rows_b, head), F32),
            pltpu.VMEM((kv_size, batch, cols), F32),
            pltpu.VMEM((batch, group, head), F32),
            pltpu.VMEM((batch, group, head), F32),
            dma((6,)),
            dma((8, inner)),
            dma((8, outer)),
            dma((2, kv_size)),
        ],
        compiler_params=pltpu.CompilerParams(collective_id=0, has_side_effects=True),
    )(live, owner, freq, x, wq, wkv, wo, keys, vals).astype(BF16)


def solution(mesh):
    return jax.shard_map(
        functools.partial(local, mesh.shape["seq"], mesh.shape["kv"]),
        mesh=mesh,
        in_specs=(
            P("dp", None),
            P("seq", "kv"),
            P("seq", "kv"),
            P("kv", "seq"),
            P("dp", "kv", "seq", None),
            P("dp", "kv", "seq", None),
            P("dp", None),
            P("dp"),
        ),
        out_specs=P("dp", "seq"),
        check_vma=False,
    )
```

```python
import functools
import math

import jax
import jax.numpy as jnp
import numpy as np
from jax import lax
from jax.experimental import pallas as pl
from jax.experimental.pallas import tpu as pltpu
from jax.sharding import PartitionSpec as P

ROPE_THETA = 500000.0
F32 = jnp.float32
BF16 = jnp.bfloat16


def gather_start(buf, rank, count, send_sem, recv_sem, peer_of):
    copies = []
    for d in range(1, count):
        j = lax.rem(rank + d, count)
        cp = pltpu.make_async_remote_copy(
            src_ref=buf.at[rank],
            dst_ref=buf.at[rank],
            send_sem=send_sem.at[d],
            recv_sem=recv_sem.at[rank],
            device_id=peer_of(j),
            device_id_type=pl.DeviceIdType.MESH,
        )
        cp.start()
        copies.append(cp)
    return copies


def gather_wait(buf, rank, count, send_sem, recv_sem, peer_of):
    for d in range(1, count):
        j = lax.rem(rank + d, count)
        pltpu.make_async_remote_copy(
            src_ref=buf.at[j],
            dst_ref=buf.at[j],
            send_sem=send_sem.at[d],
            recv_sem=recv_sem.at[j],
            device_id=peer_of(j),
            device_id_type=pl.DeviceIdType.MESH,
        ).wait_recv()


def kernel(
    n, inner, outer, kv_size, group, head,
    live, owner, freq, x_hbm, wq_hbm, wkv_hbm, wo_hbm, k_hbm, v_hbm,
    out,
    x, wq, wkv, wo, keys, vals,
    part_in, part_out, acc_all, stat_all, kv_buf, q_rows, att_rows,
    load_sem, sa, ra, sb, rb, sc, rc, sd, rd, se, re,
):
    me = lax.axis_index("seq")
    kv = lax.axis_index("kv")
    batch = x.shape[0]
    rows = wq.shape[0]
    qw = wq.shape[1]
    slots = keys.shape[2]
    plane = me // inner
    spot = lax.rem(me, inner)

    def inner_peer(j):
        return {"seq": plane * inner + j}

    def outer_peer(j):
        return {"seq": j * inner + spot}

    def seq_peer(j):
        return {"seq": j}

    def kv_peer(j):
        return {"kv": j}

    barrier = pltpu.get_barrier_semaphore()
    for d in range(1, inner):
        pl.semaphore_signal(barrier, inc=1, device_id=inner_peer(lax.rem(spot + d, inner)),
                            device_id_type=pl.DeviceIdType.MESH)
    for d in range(1, outer):
        pl.semaphore_signal(barrier, inc=1, device_id=outer_peer(lax.rem(plane + d, outer)),
                            device_id_type=pl.DeviceIdType.MESH)
    for d in range(1, kv_size):
        pl.semaphore_signal(barrier, inc=1, device_id=kv_peer(lax.rem(kv + d, kv_size)),
                            device_id_type=pl.DeviceIdType.MESH)

    first = pl.multiple_of(me * rows, rows)
    loads = [
        pltpu.make_async_copy(x_hbm.at[:, pl.ds(first, rows)], x, load_sem.at[0]),
        pltpu.make_async_copy(wq_hbm, wq, load_sem.at[1]),
        pltpu.make_async_copy(wkv_hbm, wkv, load_sem.at[2]),
        pltpu.make_async_copy(k_hbm, keys, load_sem.at[3]),
        pltpu.make_async_copy(v_hbm, vals, load_sem.at[4]),
        pltpu.make_async_copy(wo_hbm, wo, load_sem.at[5]),
    ]
    for cp in loads[:3]:
        cp.start()

    row_id = lax.broadcasted_iota(jnp.int32, (batch, head), 0)
    lane_id = lax.broadcasted_iota(jnp.int32, (batch, head), 1)
    position = jnp.zeros((batch, head), jnp.int32)
    for b in range(batch):
        own = owner[b]
        position = jnp.where(row_id == b, own * slots + live[b, own], position)
    angle = position.astype(F32) * freq[...]
    cosine = jnp.cos(angle)
    sine = jnp.sin(angle)
    sine = jnp.where(lane_id < head // 2, -sine, sine)

    def rotate(v):
        return v * cosine + pltpu.roll(v, head // 2, 1) * sine

    for cp in loads[:3]:
        cp.wait()
    for cp in loads[3:]:
        cp.start()
    xs = x[...]
    part_in[spot, :, :qw] = jnp.dot(xs, wq[...], preferred_element_type=F32)
    part_in[spot, :, qw:] = jnp.dot(xs, wkv[...], preferred_element_type=F32)
    pl.semaphore_wait(barrier, inner + outer + kv_size - 3)

    sends = gather_start(part_in, spot, inner, sa, ra, inner_peer)
    gather_wait(part_in, spot, inner, sa, ra, inner_peer)
    total = part_in[0]
    for j in range(1, inner):
        total = total + part_in[j]
    part_out[plane] = total
    sends += gather_start(part_out, plane, outer, sb, rb, outer_peer)
    gather_wait(part_out, plane, outer, sb, rb, outer_peer)
    total = part_out[0]
    for j in range(1, outer):
        total = total + part_out[j]

    for h in range(group):
        q_rows[:, h, :] = rotate(total[:, h * head:(h + 1) * head])
    key_new = rotate(total[:, qw:qw + head]).astype(BF16).astype(F32)
    value_new = total[:, qw + head:qw + 2 * head].astype(BF16).astype(F32)

    loads[3].wait()
    loads[4].wait()
    scaling = 1.0 / math.sqrt(head)
    slot_id = lax.broadcasted_iota(jnp.int32, (group, slots), 1)
    stat_lane = lax.broadcasted_iota(jnp.int32, (group, head), 1)
    stat_row = lax.broadcasted_iota(jnp.int32, (group, head), 0)
    pairs = batch * group
    stat = jnp.zeros((group, head), F32)
    accs = []
    for b in range(batch):
        q = q_rows[b].astype(BF16)
        new_score = jnp.sum(q.astype(F32) * key_new[b:b + 1], -1, keepdims=True) * scaling
        new_score = jnp.where(owner[b] == me, new_score, -jnp.inf)
        s = lax.dot_general(q, keys[b, 0], (((1,), (1,)), ((), ())), preferred_element_type=F32)
        s = jnp.where(slot_id < live[b, me], s * scaling, -jnp.inf)
        top = jnp.maximum(jnp.max(s, -1, keepdims=True), new_score)
        prob = jnp.exp(s - top).astype(BF16)
        new_prob = jnp.exp(new_score - top).astype(BF16).astype(F32)
        count = jnp.sum(prob.astype(F32), -1, keepdims=True) + new_prob
        acc = jnp.dot(prob, vals[b, 0], preferred_element_type=F32)
        accs.append(acc + new_prob * value_new[b:b + 1])
        stat = jnp.where(stat_lane == b * group + stat_row, top, stat)
        stat = jnp.where(stat_lane == pairs + b * group + stat_row, count, stat)
    stat_all[me] = jnp.sum(stat, 0, keepdims=True)
    acc_all[me] = jnp.concatenate(accs, 0).astype(BF16)

    sends += gather_start(stat_all, me, n, sd, rd, seq_peer)
    sends += gather_start(acc_all, me, n, sc, rc, seq_peer)
    gather_wait(stat_all, me, n, sd, rd, seq_peer)
    stats = stat_all[:, 0, :]
    factor = jnp.exp(stats - jnp.max(stats, 0, keepdims=True))
    whole = jnp.sum(factor * pltpu.roll(stats, head - pairs, 1), 0, keepdims=True)
    lane = lax.broadcasted_iota(jnp.int32, stats.shape, 1)
    weight = jnp.where(lane < pairs, factor / whole, 0.0).T
    gather_wait(acc_all, me, n, sc, rc, seq_peer)
    total = weight[:pairs, 0:1] * acc_all[0].astype(F32)
    for j in range(1, n):
        total = total + weight[:pairs, j:j + 1] * acc_all[j].astype(F32)
    for b in range(batch):
        att_rows[b] = total[b * group:(b + 1) * group]
    attended = jnp.concatenate([att_rows[:, h, :].astype(BF16) for h in range(group)], -1)

    loads[5].wait()
    kv_buf[kv] = jnp.dot(attended, wo[...], preferred_element_type=F32)
    sends += gather_start(kv_buf, kv, kv_size, se, re, kv_peer)
    gather_wait(kv_buf, kv, kv_size, se, re, kv_peer)
    total = kv_buf[0]
    for j in range(1, kv_size):
        total = total + kv_buf[j]
    out[...] = total
    for cp in sends:
        cp.wait_send()


def local(n, kv_size, x, wq, wkv, wo, keys, vals, live, owner):
    batch = x.shape[0]
    head = keys.shape[3]
    rows, qw = wq.shape
    group = qw // head
    cols = wo.shape[1]
    inner = 1
    while inner * inner < n and n % (inner * 2) == 0:
        inner *= 2
    outer = n // inner
    half = np.float64(ROPE_THETA) ** (-np.arange(0, head, 2, dtype=np.float64) / head)
    freq = jnp.asarray(np.concatenate([half, half]).astype(np.float32)[None, :])
    dma = pltpu.SemaphoreType.DMA
    smem = pl.BlockSpec(memory_space=pltpu.SMEM)
    vmem = pl.BlockSpec(memory_space=pltpu.VMEM)
    hbm = pl.BlockSpec(memory_space=pl.ANY)
    return pl.pallas_call(
        functools.partial(kernel, n, inner, outer, kv_size, group, head),
        out_shape=pltpu.VMEM((batch, cols), F32),
        in_specs=[smem, smem, vmem] + [hbm] * 6,
        out_specs=vmem,
        scratch_shapes=[
            pltpu.VMEM((batch, rows), BF16),
            pltpu.VMEM(wq.shape, BF16),
            pltpu.VMEM(wkv.shape, BF16),
            pltpu.VMEM(wo.shape, BF16),
            pltpu.VMEM(keys.shape, BF16),
            pltpu.VMEM(vals.shape, BF16),
            pltpu.VMEM((inner, batch, qw + wkv.shape[1]), F32),
            pltpu.VMEM((outer, batch, qw + wkv.shape[1]), F32),
            pltpu.VMEM((n, batch * group, head), BF16),
            pltpu.VMEM((n, 1, head), F32),
            pltpu.VMEM((kv_size, batch, cols), F32),
            pltpu.VMEM((batch, group, head), F32),
            pltpu.VMEM((batch, group, head), F32),
            dma((6,)),
            dma((inner,)), dma((inner,)),
            dma((outer,)), dma((outer,)),
            dma((n,)), dma((n,)),
            dma((n,)), dma((n,)),
            dma((kv_size,)), dma((kv_size,)),
        ],
        compiler_params=pltpu.CompilerParams(collective_id=0, has_side_effects=True),
    )(live, owner, freq, x, wq, wkv, wo, keys, vals).astype(BF16)


def solution(mesh):
    return jax.shard_map(
        functools.partial(local, mesh.shape["seq"], mesh.shape["kv"]),
        mesh=mesh,
        in_specs=(
            P("dp", None),
            P("seq", "kv"),
            P("seq", "kv"),
            P("kv", "seq"),
            P("dp", "kv", "seq", None),
            P("dp", "kv", "seq", None),
            P("dp", None),
            P("dp"),
        ),
        out_specs=P("dp", "seq"),
        check_vma=False,
    )
```

```python
import functools
import math

import jax
import jax.numpy as jnp
import numpy as np
from jax import lax
from jax.experimental import pallas as pl
from jax.experimental.pallas import tpu as pltpu
from jax.sharding import PartitionSpec as P

ROPE_THETA = 500000.0
F32 = jnp.float32
BF16 = jnp.bfloat16


def gather_start(buf, rank, count, send_sem, recv_sem, peer_of):
    copies = []
    for d in range(1, count):
        j = lax.rem(rank + d, count)
        cp = pltpu.make_async_remote_copy(
            src_ref=buf.at[rank],
            dst_ref=buf.at[rank],
            send_sem=send_sem.at[d],
            recv_sem=recv_sem.at[rank],
            device_id=peer_of(j),
            device_id_type=pl.DeviceIdType.MESH,
        )
        cp.start()
        copies.append(cp)
    return copies


def gather_wait(buf, rank, count, send_sem, recv_sem, peer_of):
    for d in range(1, count):
        j = lax.rem(rank + d, count)
        pltpu.make_async_remote_copy(
            src_ref=buf.at[j],
            dst_ref=buf.at[j],
            send_sem=send_sem.at[d],
            recv_sem=recv_sem.at[j],
            device_id=peer_of(j),
            device_id_type=pl.DeviceIdType.MESH,
        ).wait_recv()


def kernel(
    n, inner, outer, kv_size, group, head,
    live, owner, freq, x_hbm, wq_hbm, wkv_hbm, wo_hbm, k_hbm, v_hbm,
    out,
    x, wq, wkv, wo, keys, vals,
    part_in, part_out, acc_all, stat_all, kv_buf, q_rows, att_rows,
    load_sem, sa, ra, sb, rb, sc, rc, sd, rd, se, re, relay_sem,
):
    me = lax.axis_index("seq")
    kv = lax.axis_index("kv")
    batch = x.shape[0]
    rows = wq.shape[0]
    qw = wq.shape[1]
    slots = keys.shape[2]
    plane = me // inner
    spot = lax.rem(me, inner)

    def inner_peer(j):
        return {"seq": plane * inner + j}

    def outer_peer(j):
        return {"seq": j * inner + spot}

    def seq_peer(j):
        return {"seq": j}

    def kv_peer(j):
        return {"kv": j}

    barrier = pltpu.get_barrier_semaphore()
    for d in range(1, inner):
        pl.semaphore_signal(barrier, inc=1, device_id=inner_peer(lax.rem(spot + d, inner)),
                            device_id_type=pl.DeviceIdType.MESH)
    steps = [1 << i for i in range(outer.bit_length() - 1)]

    def across(step):
        return outer_peer(plane + step - 2 * step * lax.rem(plane // step, 2))

    for step in steps:
        pl.semaphore_signal(barrier, inc=1, device_id=across(step),
                            device_id_type=pl.DeviceIdType.MESH)
    for d in range(1, kv_size):
        pl.semaphore_signal(barrier, inc=1, device_id=kv_peer(lax.rem(kv + d, kv_size)),
                            device_id_type=pl.DeviceIdType.MESH)

    first = pl.multiple_of(me * rows, rows)
    loads = [
        pltpu.make_async_copy(x_hbm.at[:, pl.ds(first, rows)], x, load_sem.at[0]),
        pltpu.make_async_copy(wq_hbm, wq, load_sem.at[1]),
        pltpu.make_async_copy(wkv_hbm, wkv, load_sem.at[2]),
        pltpu.make_async_copy(k_hbm, keys, load_sem.at[3]),
        pltpu.make_async_copy(v_hbm, vals, load_sem.at[4]),
        pltpu.make_async_copy(wo_hbm, wo, load_sem.at[5]),
    ]
    for cp in loads[:3]:
        cp.start()

    row_id = lax.broadcasted_iota(jnp.int32, (batch, head), 0)
    lane_id = lax.broadcasted_iota(jnp.int32, (batch, head), 1)
    position = jnp.zeros((batch, head), jnp.int32)
    for b in range(batch):
        own = owner[b]
        position = jnp.where(row_id == b, own * slots + live[b, own], position)
    angle = position.astype(F32) * freq[...]
    cosine = jnp.cos(angle)
    sine = jnp.sin(angle)
    sine = jnp.where(lane_id < head // 2, -sine, sine)

    def rotate(v):
        return v * cosine + pltpu.roll(v, head // 2, 1) * sine

    for cp in loads[:3]:
        cp.wait()
    for cp in loads[3:]:
        cp.start()
    xs = x[...]
    part_in[spot, :, :qw] = jnp.dot(xs, wq[...], preferred_element_type=F32)
    part_in[spot, :, qw:] = jnp.dot(xs, wkv[...], preferred_element_type=F32)
    pl.semaphore_wait(barrier, inner - 1 + len(steps) + kv_size - 1)

    sends = gather_start(part_in, spot, inner, sa, ra, inner_peer)
    for i in range(len(steps) - 1):
        for step in steps:
            pl.semaphore_signal(relay_sem.at[i], inc=1, device_id=across(step),
                                device_id_type=pl.DeviceIdType.MESH)
        pl.semaphore_wait(relay_sem.at[i], len(steps))
    gather_wait(part_in, spot, inner, sa, ra, inner_peer)
    total = part_in[0]
    for j in range(1, inner):
        total = total + part_in[j]
    part_out[plane] = total
    sends += gather_start(part_out, plane, outer, sb, rb, outer_peer)
    gather_wait(part_out, plane, outer, sb, rb, outer_peer)
    total = part_out[0]
    for j in range(1, outer):
        total = total + part_out[j]

    for h in range(group):
        q_rows[:, h, :] = rotate(total[:, h * head:(h + 1) * head])
    key_new = rotate(total[:, qw:qw + head]).astype(BF16).astype(F32)
    value_new = total[:, qw + head:qw + 2 * head].astype(BF16).astype(F32)

    loads[3].wait()
    loads[4].wait()
    scaling = 1.0 / math.sqrt(head)
    slot_id = lax.broadcasted_iota(jnp.int32, (group, slots), 1)
    stat_lane = lax.broadcasted_iota(jnp.int32, (group, head), 1)
    stat_row = lax.broadcasted_iota(jnp.int32, (group, head), 0)
    pairs = batch * group
    stat = jnp.zeros((group, head), F32)
    accs = []
    for b in range(batch):
        q = q_rows[b].astype(BF16)
        new_score = jnp.sum(q.astype(F32) * key_new[b:b + 1], -1, keepdims=True) * scaling
        new_score = jnp.where(owner[b] == me, new_score, -jnp.inf)
        s = lax.dot_general(q, keys[b, 0], (((1,), (1,)), ((), ())), preferred_element_type=F32)
        s = jnp.where(slot_id < live[b, me], s * scaling, -jnp.inf)
        top = jnp.maximum(jnp.max(s, -1, keepdims=True), new_score)
        prob = jnp.exp(s - top).astype(BF16)
        new_prob = jnp.exp(new_score - top).astype(BF16).astype(F32)
        count = jnp.sum(prob.astype(F32), -1, keepdims=True) + new_prob
        acc = jnp.dot(prob, vals[b, 0], preferred_element_type=F32)
        accs.append(acc + new_prob * value_new[b:b + 1])
        stat = jnp.where(stat_lane == b * group + stat_row, top, stat)
        stat = jnp.where(stat_lane == pairs + b * group + stat_row, count, stat)
    stat_all[me] = jnp.sum(stat, 0, keepdims=True)
    acc_all[me] = jnp.concatenate(accs, 0).astype(BF16)

    sends += gather_start(stat_all, me, n, sd, rd, seq_peer)
    sends += gather_start(acc_all, me, n, sc, rc, seq_peer)
    gather_wait(stat_all, me, n, sd, rd, seq_peer)
    stats = stat_all[:, 0, :]
    factor = jnp.exp(stats - jnp.max(stats, 0, keepdims=True))
    whole = jnp.sum(factor * pltpu.roll(stats, head - pairs, 1), 0, keepdims=True)
    lane = lax.broadcasted_iota(jnp.int32, stats.shape, 1)
    weight = jnp.where(lane < pairs, factor / whole, 0.0).T
    gather_wait(acc_all, me, n, sc, rc, seq_peer)
    total = weight[:pairs, 0:1] * acc_all[0].astype(F32)
    for j in range(1, n):
        total = total + weight[:pairs, j:j + 1] * acc_all[j].astype(F32)
    for b in range(batch):
        att_rows[b] = total[b * group:(b + 1) * group]
    attended = jnp.concatenate([att_rows[:, h, :].astype(BF16) for h in range(group)], -1)

    loads[5].wait()
    kv_buf[kv] = jnp.dot(attended, wo[...], preferred_element_type=F32)
    sends += gather_start(kv_buf, kv, kv_size, se, re, kv_peer)
    gather_wait(kv_buf, kv, kv_size, se, re, kv_peer)
    total = kv_buf[0]
    for j in range(1, kv_size):
        total = total + kv_buf[j]
    out[...] = total
    for cp in sends:
        cp.wait_send()


def local(n, kv_size, x, wq, wkv, wo, keys, vals, live, owner):
    batch = x.shape[0]
    head = keys.shape[3]
    rows, qw = wq.shape
    group = qw // head
    cols = wo.shape[1]
    inner = 1
    while inner * inner < n and n % (inner * 2) == 0:
        inner *= 2
    outer = n // inner
    half = np.float64(ROPE_THETA) ** (-np.arange(0, head, 2, dtype=np.float64) / head)
    freq = jnp.asarray(np.concatenate([half, half]).astype(np.float32)[None, :])
    dma = pltpu.SemaphoreType.DMA
    smem = pl.BlockSpec(memory_space=pltpu.SMEM)
    vmem = pl.BlockSpec(memory_space=pltpu.VMEM)
    hbm = pl.BlockSpec(memory_space=pl.ANY)
    return pl.pallas_call(
        functools.partial(kernel, n, inner, outer, kv_size, group, head),
        out_shape=pltpu.VMEM((batch, cols), F32),
        in_specs=[smem, smem, vmem] + [hbm] * 6,
        out_specs=vmem,
        scratch_shapes=[
            pltpu.VMEM((batch, rows), BF16),
            pltpu.VMEM(wq.shape, BF16),
            pltpu.VMEM(wkv.shape, BF16),
            pltpu.VMEM(wo.shape, BF16),
            pltpu.VMEM(keys.shape, BF16),
            pltpu.VMEM(vals.shape, BF16),
            pltpu.VMEM((inner, batch, qw + wkv.shape[1]), F32),
            pltpu.VMEM((outer, batch, qw + wkv.shape[1]), F32),
            pltpu.VMEM((n, batch * group, head), BF16),
            pltpu.VMEM((n, 1, head), F32),
            pltpu.VMEM((kv_size, batch, cols), F32),
            pltpu.VMEM((batch, group, head), F32),
            pltpu.VMEM((batch, group, head), F32),
            dma((6,)),
            dma((inner,)), dma((inner,)),
            dma((outer,)), dma((outer,)),
            dma((n,)), dma((n,)),
            dma((n,)), dma((n,)),
            dma((kv_size,)), dma((kv_size,)),
            pltpu.SemaphoreType.REGULAR((max(outer.bit_length() - 2, 1),)),
        ],
        compiler_params=pltpu.CompilerParams(collective_id=0, has_side_effects=True),
    )(live, owner, freq, x, wq, wkv, wo, keys, vals).astype(BF16)


def solution(mesh):
    return jax.shard_map(
        functools.partial(local, mesh.shape["seq"], mesh.shape["kv"]),
        mesh=mesh,
        in_specs=(
            P("dp", None),
            P("seq", "kv"),
            P("seq", "kv"),
            P("kv", "seq"),
            P("dp", "kv", "seq", None),
            P("dp", "kv", "seq", None),
            P("dp", None),
            P("dp"),
        ),
        out_specs=P("dp", "seq"),
        check_vma=False,
    )
```
